32 devices in a mesh: delay: 4 (over y, core), row: 8 (over z, x).
Axes of the slice: x: 2, y: 2, z: 4, core: 2. Of those that a mesh axis runs over, the one named last changes fastest.
Arguments:
- incident: bfloat16 [64, 4096], P(None, 'row'), may hold values from -12 to 12
- onset: int32 [64], replicated, may hold values from 0 to 2
- beta: float32 [4096], P('delay'), may hold values from 0.05 to 0.5
- inverse_block: bfloat16 [4096, 4096], P('row', 'delay'), may hold values from -0.0625 to 0.0625
- delay_blocks: bfloat16 [4, 4096, 4096], P('delay', None, 'row'), may hold values from -0.09375 to 0.09375
- history_sum: float32 [4, 64, 4096], P('delay', None, 'row'), may hold values from -12 to 12
Outputs:
- currents: bfloat16 [3, 64, 4096], P(None, None, 'delay')
- carried: float32 [4, 64, 4096], P('delay', None, 'row')
The draws below stay inside these ranges and needn't reach their ends.
All inputs are finite; a program needn't handle non-finite values.
Results may differ from the reference program's by a relative error of at most 0.0056.
Values may be sent and summed in bfloat16 or wider, within the bound.
No kernel may reach another device: no remote copies, remote signals or barrier semaphores. Data moves between devices by JAX's collectives and lax.ppermute only.
A program may use at most 64 MiB of HBM per device.

```python
import math
import jax
import jax.numpy as jnp
from jax import lax

N = 4096
E = 64
STEPS = 3
DELAYS = 4


def set_ends(result, stream_key, least, largest):
    longest = result.shape.index(max(result.shape))
    spots = []
    for shift in (0, 1):
        where = [jax.random.randint(jax.random.fold_in(stream_key, axis), (), 0, length) for axis, length in enumerate(result.shape)]
        where[longest] = (where[longest] + shift) % result.shape[longest]
        spots.append(tuple(where))
    return result.at[spots[0]].set(least).at[spots[1]].set(largest)


def block_levels(stream_key, dims, cuts, least, top_value):
    loudness = 1.0
    for axis_at, shards_of in cuts:
        draws = jax.random.uniform(jax.random.fold_in(jax.random.fold_in(stream_key, 6), axis_at), (shards_of,), jnp.float32, least / len(cuts), top_value / len(cuts))
        loudness = loudness * jnp.repeat(jnp.exp(draws), dims[axis_at] // shards_of).reshape((-1,) + (1,) * (len(dims) - 1 - axis_at))
    return loudness


def noise(key, shape, deviation, most, shards=(), dtype=jnp.bfloat16):
    level = block_levels(key, shape, shards, -0.22, 0.18) if shards else 1.0
    entries = jax.random.normal(key, shape, jnp.float32) * deviation * level
    return jnp.minimum(jnp.maximum(entries, -most), most).astype(dtype)


def setup_inputs(seed: int = 0) -> dict:
    streams_of = jax.random.split(jax.random.key(seed), 7)
    incident = noise(streams_of[0], (E, N), 2.0, 12.0, ((1, 8),))
    onset = set_ends(jax.random.randint(streams_of[1], (E,), 0, STEPS), jax.random.fold_in(streams_of[1], 1), 0, STEPS - 1).astype(jnp.int32)
    beta = jnp.clip(jnp.exp(math.log(0.5) - 2.3025851 * jax.random.uniform(streams_of[2], (N,), jnp.float32) ** block_levels(streams_of[2], (N,), ((0, 4),), -0.2, 0.2)), 0.05, 0.5)
    inverse_block = noise(streams_of[3], (N, N), (2 * N) ** -0.5, 0.0625, ((0, 8), (1, 4)))
    delay_blocks = noise(streams_of[4], (DELAYS, N, N), N ** -0.5, 0.09375, ((0, 4), (2, 8)))
    history_sum = noise(streams_of[5], (DELAYS, E, N), 2.0, 12.0, ((0, 4), (2, 8)), jnp.float32)
    return dict(incident=incident, onset=onset, beta=beta, inverse_block=inverse_block, delay_blocks=delay_blocks, history_sum=history_sum)


def reference(incident, onset, beta, inverse_block, delay_blocks, history_sum):
    delay_wide = delay_blocks.astype(jnp.float32)
    incident_wide = incident.astype(jnp.float32)
    future = history_sum
    outputs = []
    for step_index in range(STEPS):
        offset_time = (step_index - onset).astype(jnp.float32)
        envelope = jnp.where(offset_time >= 0.0, jnp.exp(-(offset_time - 1.0) ** 2 / 4.0), 0.0)
        drive = incident_wide * envelope[:, None]
        residual = (drive - future[0]).astype(jnp.bfloat16)
        solved = jnp.dot(residual, inverse_block, preferred_element_type=jnp.float32)
        current = (solved / (1.0 + beta[None, :] * solved * solved)).astype(jnp.bfloat16)
        outputs.append(current)
        contrib = jnp.einsum("en,knm->kem", current.astype(jnp.float32), delay_wide, precision=lax.Precision.HIGHEST)
        future = jnp.concatenate([future[1:], jnp.zeros_like(future[:1])], axis=0) + contrib
    return jnp.stack(outputs), future
```

```python
import jax
import jax.numpy as jnp
from jax import lax
from jax.sharding import PartitionSpec as P

STEPS = 3


def bits_of(axis):
    return [1 << b for b in range(lax.axis_size(axis).bit_length() - 1)]


def swapped(value, axis, bit):
    return lax.ppermute(value, axis, [(i, i ^ bit) for i in range(lax.axis_size(axis))])


def total_over_delay(value, wires):
    for bit, wire in zip(bits_of("delay"), wires):
        other = swapped(value.astype(wire), "delay", bit)
        value = value + other.astype(value.dtype)
    return value


def summed_over_row(partial_sum):
    bits = bits_of("row")
    odd = (lax.axis_index("row") & 1) == 1
    half = partial_sum.shape[1] // 2
    low, high = partial_sum[:, :half], partial_sum[:, half:]
    other = swapped(jnp.where(odd, low, high).astype(jnp.bfloat16), "row", bits[0])
    value = jnp.where(odd, high, low) + other.astype(jnp.float32)
    for bit in bits[1:]:
        sent = value.astype(jnp.bfloat16)
        other = swapped(sent, "row", bit)
        value = sent.astype(jnp.float32) + other.astype(jnp.float32)
    return value


def joined(mine, other, second):
    return jnp.where(second, other, mine), jnp.where(second, mine, other)


def gathered_over_delay(chunk):
    place = lax.axis_index("delay")
    parts = [chunk]
    for bit in reversed(bits_of("delay")):
        second = (place & bit) != 0
        pairs = [joined(p, swapped(p, "delay", bit), second) for p in parts]
        parts = [q for pair in pairs for q in pair]
    return jnp.concatenate(parts, axis=1)


def per_device(incident, onset, beta, inverse_block, delay_blocks, history_sum):
    place = lax.axis_index("delay")
    odd = (lax.axis_index("row") & 1) == 1
    lags = lax.axis_size("delay")
    future = history_sum[0]
    matrix = delay_blocks[0]
    chunk = beta.shape[0]
    half = chunk // 2
    beta_half = jnp.where(odd, beta[half:], beta[:half])[None, :]
    wires = [jnp.float32] + [jnp.bfloat16] * (len(bits_of("delay")) - 1)
    incident_wide = incident.astype(jnp.float32)
    drives = []
    for step_index in range(STEPS):
        offset_time = (step_index - onset).astype(jnp.float32)
        envelope = jnp.where(offset_time >= 0.0, jnp.exp(-((offset_time - 1.0) ** 2) / 4.0), 0.0)
        drives.append(incident_wide * envelope[:, None])

    residual = jnp.where(place == 0, drives[0] - future, 0.0).astype(jnp.bfloat16)
    residual = total_over_delay(residual, [jnp.bfloat16] * len(wires))

    first_rows = matrix[:chunk]
    for k in range(1, lags):
        sent = lax.ppermute(matrix[k * chunk : (k + 1) * chunk], "delay", [(0, k)])
        first_rows = jnp.where(place == k, sent, first_rows)

    outputs = []
    for step_index in range(STEPS):
        partial_sum = jnp.dot(residual, inverse_block, preferred_element_type=jnp.float32)
        solved = summed_over_row(partial_sum)
        piece = (solved / (1.0 + beta_half * solved * solved)).astype(jnp.bfloat16)
        low, high = joined(piece, swapped(piece, "row", 1), odd)
        current = jnp.concatenate([low, high], axis=1)
        outputs.append(current)
        passed = lax.ppermute(future, "delay", [(i, i - 1) for i in range(1, lags)])
        if step_index + 1 < STEPS:
            addend = jnp.dot(current, first_rows, preferred_element_type=jnp.float32)
            addend = addend + jnp.where(place == 1, future, 0.0)
            total = total_over_delay(addend, wires)
            residual = (drives[step_index + 1] - total).astype(jnp.bfloat16)
        gathered = gathered_over_delay(current)
        future = passed + jnp.dot(gathered, matrix, preferred_element_type=jnp.float32)
    return (jnp.stack(outputs), future[None])


def solution(mesh):
    placed = (
        P(None, "row"),
        P(),
        P("delay"),
        P("row", "delay"),
        P("delay", None, "row"),
        P("delay", None, "row"),
    )
    return jax.shard_map(
        per_device,
        mesh=mesh,
        in_specs=placed,
        out_specs=(P(None, None, "delay"), P("delay", None, "row")),
        check_vma=False,
    )
```

```python
import jax
import jax.numpy as jnp
from jax import lax
from jax.sharding import PartitionSpec as P


STEPS = 3


def bits_of(axis):
    return [1 << b for b in range(lax.axis_size(axis).bit_length() - 1)]


def swapped(value, axis, bit):
    return lax.ppermute(value, axis, [(i, i ^ bit) for i in range(lax.axis_size(axis))])


def swapped_both(value, place_bit, row_bit):
    rows = lax.axis_size("row")
    count = rows * lax.axis_size("delay")
    flip = place_bit * rows + row_bit
    return lax.ppermute(value, ("delay", "row"), [(i, i ^ flip) for i in range(count)])


def total_over_delay(value, wires):
    for bit, wire in zip(bits_of("delay"), wires):
        other = swapped(value.astype(wire), "delay", bit)
        value = value + other.astype(value.dtype)
    return value


def summed_over_row(partial_sum):
    bits = bits_of("row")
    odd = (lax.axis_index("row") & 1) == 1
    half = partial_sum.shape[1] // 2
    low, high = partial_sum[:, :half], partial_sum[:, half:]
    other = swapped(jnp.where(odd, low, high).astype(jnp.bfloat16), "row", bits[0])
    value = jnp.where(odd, high, low) + other.astype(jnp.float32)
    for bit in bits[1:]:
        sent = value.astype(jnp.bfloat16)
        other = swapped(sent, "row", bit)
        value = sent.astype(jnp.float32) + other.astype(jnp.float32)
    return value


def joined(mine, other, second):
    return jnp.where(second, other, mine), jnp.where(second, mine, other)


def columns(mine, other, second):
    return jnp.concatenate(joined(mine, other, second), axis=1)


def spread(parts, bits):
    place = lax.axis_index("delay")
    for bit in bits:
        second = (place & bit) != 0
        pairs = [joined(p, swapped(p, "delay", bit), second) for p in parts]
        parts = [q for pair in pairs for q in pair]
    return jnp.concatenate(parts, axis=1)


def after(value, token):
    return lax.optimization_barrier((value, token))[0]


def steps(incident, onset, beta, inverse_block, delay_blocks, history_sum):
    place = lax.axis_index("delay")
    odd = (lax.axis_index("row") & 1) == 1
    lags = lax.axis_size("delay")
    place_bits = bits_of("delay")
    top = place_bits[-1]
    future = history_sum[0]
    matrix = delay_blocks[0]
    chunk = beta.shape[0]
    half = chunk // 2
    beta_half = jnp.where(odd, beta[half:], beta[:half])[None, :]
    wires = [jnp.float32] + [jnp.bfloat16] * (len(place_bits) - 1)
    incident_wide = incident.astype(jnp.float32)
    drives = []
    for step_index in range(STEPS):
        offset_time = (step_index - onset).astype(jnp.float32)
        envelope = jnp.where(offset_time >= 0.0, jnp.exp(-((offset_time - 1.0) ** 2) / 4.0), 0.0)
        drives.append(incident_wide * envelope[:, None])

    residual = jnp.where(place == 0, drives[0] - future, 0.0).astype(jnp.bfloat16)
    first_residual = residual
    residual = total_over_delay(residual, [jnp.bfloat16] * len(wires))

    first_rows = matrix[:chunk]
    for k in reversed(range(1, lags)):
        rows = after(matrix, first_residual[:8, :k])[k * chunk : (k + 1) * chunk]
        sent = lax.ppermute(rows, "delay", [(0, k)])
        first_rows = lax.optimization_barrier(jnp.where(place == k, sent, first_rows))

    outputs = []
    for step_index in range(STEPS):
        partial_sum = jnp.dot(residual, inverse_block, preferred_element_type=jnp.float32)
        solved = summed_over_row(partial_sum)
        piece = (solved / (1.0 + beta_half * solved * solved)).astype(jnp.bfloat16)
        passed = lax.ppermute(future, "delay", [(i, i - 1) for i in range(1, lags)])
        if step_index + 1 < STEPS:
            current = columns(piece, swapped(piece, "row", 1), odd)
            addend = jnp.dot(current, first_rows, preferred_element_type=jnp.float32)
            addend = addend + jnp.where(place == 1, future, 0.0)
            total = total_over_delay(addend, wires)
            residual = (drives[step_index + 1] - total).astype(jnp.bfloat16)
            gathered = spread([current], reversed(place_bits))
        else:
            far = (place & top) != 0
            both = swapped_both(piece, top, 1)
            near = swapped(piece, "row", 1)
            side = swapped(piece, "delay", top)
            current = columns(piece, near, odd)
            parts = list(joined(current, columns(side, both, odd), far))
            gathered = spread(parts, reversed(place_bits[:-1]))
        outputs.append(current)
        contribution = jnp.dot(gathered, matrix, preferred_element_type=jnp.float32)
        future = passed + contribution
    return (jnp.stack(outputs), future[None])


def solution(mesh):
    placed = (
        P(None, "row"),
        P(),
        P("delay"),
        P("row", "delay"),
        P("delay", None, "row"),
        P("delay", None, "row"),
    )
    return jax.shard_map(
        steps,
        mesh=mesh,
        in_specs=placed,
        out_specs=(P(None, None, "delay"), P("delay", None, "row")),
        check_vma=False,
    )
```

```python
import jax
import jax.numpy as jnp
from jax import lax
from jax.experimental import pallas as pl
from jax.experimental.pallas import tpu as pltpu
from jax.sharding import PartitionSpec as P


STEPS = 3


def bits_of(axis):
    return [1 << b for b in range(lax.axis_size(axis).bit_length() - 1)]


def swapped(value, axis, bit):
    return lax.ppermute(value, axis, [(i, i ^ bit) for i in range(lax.axis_size(axis))])


def swapped_both(value, place_bit, row_bit):
    rows = lax.axis_size("row")
    count = rows * lax.axis_size("delay")
    flip = place_bit * rows + row_bit
    return lax.ppermute(value, ("delay", "row"), [(i, i ^ flip) for i in range(count)])


def total_over_delay(value, wires):
    for bit, wire in zip(bits_of("delay"), wires):
        other = swapped(value.astype(wire), "delay", bit)
        value = value + other.astype(value.dtype)
    return value


def summed_over_row(partial_sum):
    bits = bits_of("row")
    odd = (lax.axis_index("row") & 1) == 1
    half = partial_sum.shape[1] // 2
    low, high = partial_sum[:, :half], partial_sum[:, half:]
    other = swapped(jnp.where(odd, low, high).astype(jnp.bfloat16), "row", bits[0])
    value = jnp.where(odd, high, low) + other.astype(jnp.float32)
    for bit in bits[1:]:
        sent = value.astype(jnp.bfloat16)
        other = swapped(sent, "row", bit)
        value = sent.astype(jnp.float32) + other.astype(jnp.float32)
    return value


def joined(mine, other, second):
    return jnp.where(second, other, mine), jnp.where(second, mine, other)


def columns(mine, other, second):
    return jnp.concatenate(joined(mine, other, second), axis=1)


def spread(parts, bits):
    place = lax.axis_index("delay")
    for bit in bits:
        second = (place & bit) != 0
        pairs = [joined(p, swapped(p, "delay", bit), second) for p in parts]
        parts = [q for pair in pairs for q in pair]
    return jnp.concatenate(parts, axis=1)


def cut_in_rows(matrix, chunk, count):
    def copy_rows(rows, *rest):
        copied, done = rest[:-1], rest[-1]
        copies = [
            pltpu.make_async_copy(rows.at[pl.ds(k * chunk, chunk)], copied[k - 1], done.at[k - 1])
            for k in range(1, count)
        ]
        for copy in copies:
            copy.start()
        for copy in copies:
            copy.wait()

    shape = jax.ShapeDtypeStruct((chunk, matrix.shape[1]), matrix.dtype)
    return pl.pallas_call(
        copy_rows,
        in_specs=[pl.BlockSpec(memory_space=pl.ANY)],
        out_specs=[pl.BlockSpec(memory_space=pl.ANY)] * (count - 1),
        out_shape=[shape] * (count - 1),
        scratch_shapes=[pltpu.SemaphoreType.DMA((count - 1,))],
        compiler_params=pltpu.CompilerParams(vmem_limit_bytes=1 << 20),
        name="cut_rows",
    )(matrix)


def steps(incident, onset, beta, inverse_block, delay_blocks, history_sum):
    place = lax.axis_index("delay")
    odd = (lax.axis_index("row") & 1) == 1
    lags = lax.axis_size("delay")
    place_bits = bits_of("delay")
    top = place_bits[-1]
    future = history_sum[0]
    matrix = delay_blocks[0]
    chunk = beta.shape[0]
    half = chunk // 2
    beta_half = jnp.where(odd, beta[half:], beta[:half])[None, :]
    wires = [jnp.float32] + [jnp.bfloat16] * (len(place_bits) - 1)
    incident_wide = incident.astype(jnp.float32)
    drives = []
    for step_index in range(STEPS):
        offset_time = (step_index - onset).astype(jnp.float32)
        envelope = jnp.where(offset_time >= 0.0, jnp.exp(-((offset_time - 1.0) ** 2) / 4.0), 0.0)
        drives.append(incident_wide * envelope[:, None])

    residual = jnp.where(place == 0, drives[0] - future, 0.0).astype(jnp.bfloat16)
    residual = total_over_delay(residual, [jnp.bfloat16] * len(wires))

    dealt = {}
    cut = cut_in_rows(matrix, chunk, lags)
    for k in range(1, lags):
        dealt[k] = lax.ppermute(cut[k - 1], "delay", [(0, k)])
    first_rows = matrix[:chunk]
    for k in [1] + list(reversed(range(2, lags))):
        first_rows = lax.optimization_barrier(jnp.where(place == k, dealt[k], first_rows))

    outputs = []
    for step_index in range(STEPS):
        partial_sum = jnp.dot(residual, inverse_block, preferred_element_type=jnp.float32)
        solved = summed_over_row(partial_sum)
        piece = (solved / (1.0 + beta_half * solved * solved)).astype(jnp.bfloat16)
        passed = lax.ppermute(future, "delay", [(i, i - 1) for i in range(1, lags)])
        if step_index + 1 < STEPS:
            current = columns(piece, swapped(piece, "row", 1), odd)
            addend = jnp.dot(current, first_rows, preferred_element_type=jnp.float32)
            addend = addend + jnp.where(place == 1, future, 0.0)
            total = total_over_delay(addend, wires)
            residual = (drives[step_index + 1] - total).astype(jnp.bfloat16)
            gathered = spread([current], reversed(place_bits))
        else:
            far = (place & top) != 0
            both = swapped_both(piece, top, 1)
            near = swapped(piece, "row", 1)
            side = swapped(piece, "delay", top)
            current = columns(piece, near, odd)
            parts = list(joined(current, columns(side, both, odd), far))
            gathered = spread(parts, reversed(place_bits[:-1]))
        outputs.append(current)
        contribution = jnp.dot(gathered, matrix, preferred_element_type=jnp.float32)
        future = passed + contribution
    return (jnp.stack(outputs), future[None])


def solution(mesh):
    placed = (
        P(None, "row"),
        P(),
        P("delay"),
        P("row", "delay"),
        P("delay", None, "row"),
        P("delay", None, "row"),
    )
    return jax.shard_map(
        steps,
        mesh=mesh,
        in_specs=placed,
        out_specs=(P(None, None, "delay"), P("delay", None, "row")),
        check_vma=False,
    )
```

```python
import jax
import jax.numpy as jnp
from jax import lax
from jax.experimental import pallas as pl
from jax.experimental.pallas import tpu as pltpu
from jax.sharding import PartitionSpec as P


STEPS = 3


def bits_of(axis):
    return [1 << b for b in range(lax.axis_size(axis).bit_length() - 1)]


def swapped(value, axis, bit):
    return lax.ppermute(value, axis, [(i, i ^ bit) for i in range(lax.axis_size(axis))])


def swapped_both(value, place_bit, row_bit):
    rows = lax.axis_size("row")
    count = rows * lax.axis_size("delay")
    flip = place_bit * rows + row_bit
    return lax.ppermute(value, ("delay", "row"), [(i, i ^ flip) for i in range(count)])


def total_over_delay(value, wires):
    for bit, wire in zip(bits_of("delay"), wires):
        other = swapped(value.astype(wire), "delay", bit)
        value = value + other.astype(value.dtype)
    return value


def summed_over_row(partial_sum):
    bits = bits_of("row")
    odd = (lax.axis_index("row") & 1) == 1
    half = partial_sum.shape[1] // 2
    low, high = partial_sum[:, :half], partial_sum[:, half:]
    other = swapped(jnp.where(odd, low, high).astype(jnp.bfloat16), "row", bits[0])
    value = jnp.where(odd, high, low) + other.astype(jnp.float32)
    for bit in bits[1:]:
        sent = value.astype(jnp.bfloat16)
        other = swapped(sent, "row", bit)
        value = sent.astype(jnp.float32) + other.astype(jnp.float32)
    return value


def joined(mine, other, second):
    return jnp.where(second, other, mine), jnp.where(second, mine, other)


def columns(mine, other, second):
    return jnp.concatenate(joined(mine, other, second), axis=1)


def spread(parts, bits):
    place = lax.axis_index("delay")
    for bit in bits:
        second = (place & bit) != 0
        pairs = [joined(p, swapped(p, "delay", bit), second) for p in parts]
        parts = [q for pair in pairs for q in pair]
    return jnp.concatenate(parts, axis=1)


def cut_in_rows(matrix, chunk, count):
    def copy_rows(rows, *rest):
        copied, done = rest[:-1], rest[-1]
        copies = [
            pltpu.make_async_copy(rows.at[pl.ds(k * chunk, chunk)], copied[k - 1], done.at[k - 1])
            for k in range(1, count)
        ]
        for copy in copies:
            copy.start()
        for copy in copies:
            copy.wait()

    shape = jax.ShapeDtypeStruct((chunk, matrix.shape[1]), matrix.dtype)
    return pl.pallas_call(
        copy_rows,
        in_specs=[pl.BlockSpec(memory_space=pl.ANY)],
        out_specs=[pl.BlockSpec(memory_space=pl.ANY)] * (count - 1),
        out_shape=[shape] * (count - 1),
        scratch_shapes=[pltpu.SemaphoreType.DMA((count - 1,))],
        compiler_params=pltpu.CompilerParams(vmem_limit_bytes=1 << 20),
        name="cut_rows",
    )(matrix)


def deal_pairs(k, lags):
    target = {i: i ^ 1 for i in range(lags)}
    if k > 1:
        target.update({0: k, k: k ^ 1, k ^ 1: 1, 1: 0})
    return list(target.items())


def steps(incident, onset, beta, inverse_block, delay_blocks, history_sum):
    place = lax.axis_index("delay")
    odd = (lax.axis_index("row") & 1) == 1
    lags = lax.axis_size("delay")
    place_bits = bits_of("delay")
    top = place_bits[-1]
    future = history_sum[0]
    matrix = delay_blocks[0]
    chunk = beta.shape[0]
    half = chunk // 2
    beta_half = jnp.where(odd, beta[half:], beta[:half])[None, :]
    wires = [jnp.float32] + [jnp.bfloat16] * (len(place_bits) - 1)
    incident_wide = incident.astype(jnp.float32)
    drives = []
    for step_index in range(STEPS):
        offset_time = (step_index - onset).astype(jnp.float32)
        envelope = jnp.where(offset_time >= 0.0, jnp.exp(-((offset_time - 1.0) ** 2) / 4.0), 0.0)
        drives.append(incident_wide * envelope[:, None])

    residual = jnp.where(place == 0, drives[0] - future, 0.0).astype(jnp.bfloat16)
    residual = total_over_delay(residual, [jnp.bfloat16] * len(wires))

    dealt = {}
    cut = cut_in_rows(matrix, chunk, lags)
    for k in range(1, lags):
        dealt[k] = lax.ppermute(cut[k - 1], "delay", deal_pairs(k, lags))
    first_rows = matrix[:chunk]
    for k in [1] + list(reversed(range(2, lags))):
        first_rows = lax.optimization_barrier(jnp.where(place == k, dealt[k], first_rows))

    outputs = []
    for step_index in range(STEPS):
        partial_sum = jnp.dot(residual, inverse_block, preferred_element_type=jnp.float32)
        solved = summed_over_row(partial_sum)
        piece = (solved / (1.0 + beta_half * solved * solved)).astype(jnp.bfloat16)
        passed = lax.ppermute(future, "delay", [(i, i - 1) for i in range(1, lags)])
        if step_index + 1 < STEPS:
            current = columns(piece, swapped(piece, "row", 1), odd)
            addend = jnp.dot(current, first_rows, preferred_element_type=jnp.float32)
            addend = addend + jnp.where(place == 1, future, 0.0)
            total = total_over_delay(addend, wires)
            residual = (drives[step_index + 1] - total).astype(jnp.bfloat16)
            gathered = spread([current], reversed(place_bits))
        else:
            far = (place & top) != 0
            both = swapped_both(piece, top, 1)
            near = swapped(piece, "row", 1)
            side = swapped(piece, "delay", top)
            current = columns(piece, near, odd)
            parts = list(joined(current, columns(side, both, odd), far))
            gathered = spread(parts, reversed(place_bits[:-1]))
        outputs.append(current)
        contribution = jnp.dot(gathered, matrix, preferred_element_type=jnp.float32)
        future = passed + contribution
    return (jnp.stack(outputs), future[None])


def solution(mesh):
    placed = (
        P(None, "row"),
        P(),
        P("delay"),
        P("row", "delay"),
        P("delay", None, "row"),
        P("delay", None, "row"),
    )
    return jax.shard_map(
        steps,
        mesh=mesh,
        in_specs=placed,
        out_specs=(P(None, None, "delay"), P("delay", None, "row")),
        check_vma=False,
    )
```

```python
import jax
import jax.numpy as jnp
from jax import lax
from jax.experimental import pallas as pl
from jax.experimental.pallas import tpu as pltpu
from jax.sharding import PartitionSpec as P


STEPS = 3


def bits_of(axis):
    return [1 << b for b in range(lax.axis_size(axis).bit_length() - 1)]


def swapped(value, axis, bit):
    return lax.ppermute(value, axis, [(i, i ^ bit) for i in range(lax.axis_size(axis))])


def swapped_both(value, place_bit, row_bit):
    rows = lax.axis_size("row")
    count = rows * lax.axis_size("delay")
    flip = place_bit * rows + row_bit
    return lax.ppermute(value, ("delay", "row"), [(i, i ^ flip) for i in range(count)])


def total_over_delay(value, wires):
    for bit, wire in zip(bits_of("delay"), wires):
        other = swapped(value.astype(wire), "delay", bit)
        value = value + other.astype(value.dtype)
    return value


def summed_over_row(partial_sum):
    bits = bits_of("row")
    odd = (lax.axis_index("row") & 1) == 1
    half = partial_sum.shape[1] // 2
    low, high = partial_sum[:, :half], partial_sum[:, half:]
    other = swapped(jnp.where(odd, low, high).astype(jnp.bfloat16), "row", bits[0])
    value = jnp.where(odd, high, low) + other.astype(jnp.float32)
    for bit in bits[1:]:
        sent = value.astype(jnp.bfloat16)
        other = swapped(sent, "row", bit)
        value = sent.astype(jnp.float32) + other.astype(jnp.float32)
    return value


def joined(mine, other, second):
    return jnp.where(second, other, mine), jnp.where(second, mine, other)


def columns(mine, other, second):
    return jnp.concatenate(joined(mine, other, second), axis=1)


def spread(parts, bits):
    place = lax.axis_index("delay")
    for bit in bits:
        second = (place & bit) != 0
        pairs = [joined(p, swapped(p, "delay", bit), second) for p in parts]
        parts = [q for pair in pairs for q in pair]
    return jnp.concatenate(parts, axis=1)


def cut_in_rows(matrix, chunk, count):
    def copy_rows(rows, *rest):
        copied, done = rest[:-1], rest[-1]
        copies = [
            pltpu.make_async_copy(rows.at[pl.ds(k * chunk, chunk)], copied[k - 1], done.at[k - 1])
            for k in range(1, count)
        ]
        for copy in copies:
            copy.start()
        for copy in copies:
            copy.wait()

    shape = jax.ShapeDtypeStruct((chunk, matrix.shape[1]), matrix.dtype)
    return pl.pallas_call(
        copy_rows,
        in_specs=[pl.BlockSpec(memory_space=pl.ANY)],
        out_specs=[pl.BlockSpec(memory_space=pl.ANY)] * (count - 1),
        out_shape=[shape] * (count - 1),
        scratch_shapes=[pltpu.SemaphoreType.DMA((count - 1,))],
        compiler_params=pltpu.CompilerParams(vmem_limit_bytes=1 << 20),
        name="cut_rows",
    )(matrix)


def deal_pairs(k, lags):
    target = {i: i ^ 1 for i in range(lags)}
    if k > 1:
        target.update({0: k, k: k ^ 1, k ^ 1: 1, 1: 0})
    return list(target.items())


def steps(incident, onset, beta, inverse_block, delay_blocks, history_sum):
    place = lax.axis_index("delay")
    odd = (lax.axis_index("row") & 1) == 1
    lags = lax.axis_size("delay")
    place_bits = bits_of("delay")
    top = place_bits[-1]
    future = history_sum[0]
    matrix = delay_blocks[0]
    chunk = beta.shape[0]
    half = chunk // 2
    beta_half = jnp.where(odd, beta[half:], beta[:half])[None, :]
    wires = [jnp.float32] + [jnp.bfloat16] * (len(place_bits) - 1)
    incident_wide = incident.astype(jnp.float32)
    drives = []
    for step_index in range(STEPS):
        offset_time = (step_index - onset).astype(jnp.float32)
        envelope = jnp.where(offset_time >= 0.0, jnp.exp(-((offset_time - 1.0) ** 2) / 4.0), 0.0)
        drives.append(incident_wide * envelope[:, None])

    residual = jnp.where(place == 0, drives[0] - future, 0.0).astype(jnp.bfloat16)
    for bit in reversed(place_bits):
        residual = residual + swapped(residual, "delay", bit)

    dealt = {}
    cut = cut_in_rows(matrix, chunk, lags)
    for k in range(1, lags):
        dealt[k] = lax.ppermute(cut[k - 1], "delay", deal_pairs(k, lags))
    first_rows = matrix[:chunk]
    for k in [1] + list(reversed(range(2, lags))):
        first_rows = lax.optimization_barrier(jnp.where(place == k, dealt[k], first_rows))

    outputs = []
    for step_index in range(STEPS):
        partial_sum = jnp.dot(residual, inverse_block, preferred_element_type=jnp.float32)
        solved = summed_over_row(partial_sum)
        piece = (solved / (1.0 + beta_half * solved * solved)).astype(jnp.bfloat16)
        passed = lax.ppermute(future, "delay", [(i, (i - 1) % lags) for i in range(lags)])
        passed = jnp.where(place == lags - 1, 0.0, passed)
        if step_index + 1 < STEPS:
            current = columns(piece, swapped(piece, "row", 1), odd)
            addend = jnp.dot(current, first_rows, preferred_element_type=jnp.float32)
            addend = addend + jnp.where(place == 1, future, 0.0)
            total = total_over_delay(addend, wires)
            residual = (drives[step_index + 1] - total).astype(jnp.bfloat16)
            gathered = spread([current], reversed(place_bits))
        else:
            far = (place & top) != 0
            both = swapped_both(piece, top, 1)
            near = swapped(piece, "row", 1)
            side = swapped(piece, "delay", top)
            current = columns(piece, near, odd)
            parts = list(joined(current, columns(side, both, odd), far))
            gathered = spread(parts, reversed(place_bits[:-1]))
        outputs.append(current)
        contribution = jnp.dot(gathered, matrix, preferred_element_type=jnp.float32)
        future = passed + contribution
    return (jnp.stack(outputs), future[None])


def solution(mesh):
    placed = (
        P(None, "row"),
        P(),
        P("delay"),
        P("row", "delay"),
        P("delay", None, "row"),
        P("delay", None, "row"),
    )
    return jax.shard_map(
        steps,
        mesh=mesh,
        in_specs=placed,
        out_specs=(P(None, None, "delay"), P("delay", None, "row")),
        check_vma=False,
    )
```

```python
import jax
import jax.numpy as jnp
from jax import lax
from jax.experimental import pallas as pl
from jax.experimental.pallas import tpu as pltpu
from jax.sharding import PartitionSpec as P


STEPS = 3


def bits_of(axis):
    return [1 << b for b in range(lax.axis_size(axis).bit_length() - 1)]


def swapped(value, axis, bit):
    return lax.ppermute(value, axis, [(i, i ^ bit) for i in range(lax.axis_size(axis))])


def swapped_both(value, place_bit, row_bit):
    rows = lax.axis_size("row")
    count = rows * lax.axis_size("delay")
    flip = place_bit * rows + row_bit
    return lax.ppermute(value, ("delay", "row"), [(i, i ^ flip) for i in range(count)])


def total_over_delay(value, wires):
    for bit, wire in zip(bits_of("delay"), wires):
        other = swapped(value.astype(wire), "delay", bit)
        value = value + other.astype(value.dtype)
    return value


def summed_over_row(partial_sum):
    bits = bits_of("row")
    odd = (lax.axis_index("row") & 1) == 1
    half = partial_sum.shape[1] // 2
    low, high = partial_sum[:, :half], partial_sum[:, half:]
    other = swapped(jnp.where(odd, low, high).astype(jnp.bfloat16), "row", bits[0])
    value = jnp.where(odd, high, low) + other.astype(jnp.float32)
    for bit in bits[1:]:
        sent = value.astype(jnp.bfloat16)
        other = swapped(sent, "row", bit)
        value = sent.astype(jnp.float32) + other.astype(jnp.float32)
    return value


def joined(mine, other, second):
    return jnp.where(second, other, mine), jnp.where(second, mine, other)


def columns(mine, other, second):
    return jnp.concatenate(joined(mine, other, second), axis=1)


def spread(parts, bits):
    place = lax.axis_index("delay")
    for bit in bits:
        second = (place & bit) != 0
        pairs = [joined(p, swapped(p, "delay", bit), second) for p in parts]
        parts = [q for pair in pairs for q in pair]
    return jnp.concatenate(parts, axis=1)


def cut_in_rows(matrix, chunk, wanted):
    def copy_rows(rows, *rest):
        copied, done = rest[:-1], rest[-1]
        copies = [
            pltpu.make_async_copy(rows.at[pl.ds(k * chunk, chunk)], copied[n], done.at[n])
            for n, k in enumerate(wanted)
        ]
        for copy in copies:
            copy.start()
        for copy in copies:
            copy.wait()

    shape = jax.ShapeDtypeStruct((chunk, matrix.shape[1]), matrix.dtype)
    return pl.pallas_call(
        copy_rows,
        in_specs=[pl.BlockSpec(memory_space=pl.ANY)],
        out_specs=[pl.BlockSpec(memory_space=pl.ANY)] * len(wanted),
        out_shape=[shape] * len(wanted),
        scratch_shapes=[pltpu.SemaphoreType.DMA((len(wanted),))],
        compiler_params=pltpu.CompilerParams(vmem_limit_bytes=1 << 20),
    )(matrix)


def deal_pairs(k, lags):
    target = {i: i ^ 1 for i in range(lags)}
    if k > 1:
        target.update({0: k, k: k ^ 1, k ^ 1: 1, 1: 0})
    return list(target.items())


def steps(incident, onset, beta, inverse_block, delay_blocks, history_sum):
    place = lax.axis_index("delay")
    odd = (lax.axis_index("row") & 1) == 1
    lags = lax.axis_size("delay")
    place_bits = bits_of("delay")
    top = place_bits[-1]
    future = history_sum[0]
    matrix = delay_blocks[0]
    chunk = beta.shape[0]
    half = chunk // 2
    beta_half = jnp.where(odd, beta[half:], beta[:half])[None, :]
    wires = [jnp.float32] + [jnp.bfloat16] * (len(place_bits) - 1)
    incident_wide = incident.astype(jnp.float32)
    drives = []
    for step_index in range(STEPS):
        offset_time = (step_index - onset).astype(jnp.float32)
        envelope = jnp.where(offset_time >= 0.0, jnp.exp(-((offset_time - 1.0) ** 2) / 4.0), 0.0)
        drives.append(incident_wide * envelope[:, None])

    residual = jnp.where(place == 0, drives[0] - future, 0.0).astype(jnp.bfloat16)
    for bit in reversed(place_bits):
        residual = residual + swapped(residual, "delay", bit)

    dealt = {}
    others = [1] + list(range(3, lags))
    cut = dict(zip(others, cut_in_rows(matrix, chunk, others)))
    cut[2] = cut_in_rows(matrix, chunk, [2])[0]
    for k in range(1, lags):
        dealt[k] = lax.ppermute(cut[k], "delay", deal_pairs(k, lags))
    first_rows = matrix[:chunk]
    for k in range(1, lags):
        first_rows = lax.optimization_barrier(jnp.where(place == k, dealt[k], first_rows))

    outputs = []
    for step_index in range(STEPS):
        partial_sum = jnp.dot(residual, inverse_block, preferred_element_type=jnp.float32)
        solved = summed_over_row(partial_sum)
        piece = (solved / (1.0 + beta_half * solved * solved)).astype(jnp.bfloat16)
        passed = lax.ppermute(future, "delay", [(i, (i - 1) % lags) for i in range(lags)])
        passed = jnp.where(place == lags - 1, 0.0, passed)
        if step_index + 1 < STEPS:
            current = columns(piece, swapped(piece, "row", 1), odd)
            addend = jnp.dot(current, first_rows, preferred_element_type=jnp.float32)
            addend = addend + jnp.where(place == 1, future, 0.0)
            total = total_over_delay(addend, wires)
            residual = (drives[step_index + 1] - total).astype(jnp.bfloat16)
            gathered = spread([current], reversed(place_bits))
        else:
            far = (place & top) != 0
            both = swapped_both(piece, top, 1)
            near = swapped(piece, "row", 1)
            side = swapped(piece, "delay", top)
            current = columns(piece, near, odd)
            parts = list(joined(current, columns(side, both, odd), far))
            gathered = spread(parts, reversed(place_bits[:-1]))
        outputs.append(current)
        contribution = jnp.dot(gathered, matrix, preferred_element_type=jnp.float32)
        future = passed + contribution
    return (jnp.stack(outputs), future[None])


def solution(mesh):
    placed = (
        P(None, "row"),
        P(),
        P("delay"),
        P("row", "delay"),
        P("delay", None, "row"),
        P("delay", None, "row"),
    )
    return jax.shard_map(
        steps,
        mesh=mesh,
        in_specs=placed,
        out_specs=(P(None, None, "delay"), P("delay", None, "row")),
        check_vma=False,
    )
```
